768 devices in a mesh: section: 12 (over z_lo, core), tensor: 8 (over y), dp: 8 (over x, z_hi).
Axes of the slice: x: 4, y: 8, z: 12 (z_hi: 2, z_lo: 6; z = z_hi * 6 + z_lo), core: 2. Of those that a mesh axis runs over, the one named last changes fastest.
Arguments:
- residuals: bfloat16 [12, 8, 2, 128, 8192], P('section', 'dp', None, 'tensor'), may hold values from -6 to 6
- norm_gain: bfloat16 [12, 8192], P('section'), may hold values from 0.5 to 1.5
- projection: bfloat16 [12, 8192, 8, 2, 128], P('section', None, 'tensor'), may hold values from -0.0625 to 0.0625
- queries: bfloat16 [12, 8, 2, 128, 8, 1024], P('section', 'dp', None, None, 'tensor'), may hold values from -48 to 48
- output_grad: bfloat16 [12, 8, 2, 128, 8, 1024], P('section', 'dp', None, None, 'tensor'), may hold values from -6 to 6
- section_cotangent: bfloat16 [12, 8, 128, 8192], P('section', 'dp', 'tensor'), may hold values from -6 to 6
- loss_cotangent: bfloat16 [8, 128, 8192], P('dp', 'tensor'), may hold values from -6 to 6
- lengths: int32 [12, 8, 2], P('section', 'dp'), may hold values from 64 to 128
- segments: int32 [12, 8, 2, 128], P('section', 'dp'), may hold values from 0 to 2, never falling along the last dimension, each value on 1 to 64 neighbouring positions
Outputs:
- query_grad: bfloat16 [12, 8, 2, 128, 8, 1024], P('section', 'dp', None, None, 'tensor')
- residual_grad: bfloat16 [12, 8, 128, 8192], P('section', 'dp', 'tensor')
- projection_grad: bfloat16 [12, 8192, 8, 2, 128], P('section', 'dp', 'tensor')
The draws below stay inside these ranges and needn't reach their ends.
All inputs are finite; a program needn't handle non-finite values.
Results may differ from the reference program's by a relative error of at most 0.015.
Values may be sent and summed in bfloat16 or wider, within the bound.
No kernel may reach another device: no remote copies, remote signals or barrier semaphores. Data moves between devices by JAX's collectives and lax.ppermute only.
A program may use at most 64 MiB of HBM per device.

```python
import math
import jax
import jax.numpy as jnp
import numpy as np
from jax import lax

D = 8192
HD = 128
GROUP = 8
KVH = 8
SEQ = 128
TICKS = 2
SECTIONS = 12
REPLICAS = 8


def draw_queries(key, part):
    shape = (SECTIONS, REPLICAS, TICKS, SEQ, KVH, GROUP * HD)
    base = jnp.clip(jax.random.normal(jax.random.fold_in(key, 11), shape, jnp.float32), -6.0, 6.0)
    return base.astype(jnp.bfloat16)


def set_ends(drawn, stream_key, least, high):
    longest = drawn.shape.index(max(drawn.shape))
    spots = []
    for shift in (0, 1):
        where = [jax.random.randint(jax.random.fold_in(stream_key, axis), (), 0, length) for axis, length in enumerate(drawn.shape)]
        where[longest] = (where[longest] + shift) % drawn.shape[longest]
        spots.append(tuple(where))
    return drawn.at[spots[0]].set(least).at[spots[1]].set(high)


def steps_of(stream_key, dims, cuts, least, top_value):
    factor_of, own = 1.0, jax.random.fold_in(stream_key, 6)
    for axis_at, parts in cuts:
        heights = jnp.exp(jax.random.uniform(jax.random.fold_in(own, axis_at), (parts,), jnp.float32, least / len(cuts), top_value / len(cuts)))
        factor_of = factor_of * jnp.repeat(heights, dims[axis_at] // parts).reshape([-1 if axis == axis_at else 1 for axis in range(len(dims))])
    return factor_of


def length_profile(count, total, reach, skew):
    weights = [(1 << 20) // math.isqrt(grade ** skew) + 1 for grade in range(2, count + 1)]
    surplus, holding = total - reach - (count - 1), [1] * (count - 1)
    while surplus > 0:
        movable = [i for i in range(count - 1) if holding[i] < reach]
        whole, budget = sum([weights[i] for i in movable]), surplus
        for i in movable:
            addition = min(reach - holding[i], max(1, budget * weights[i] // whole), surplus)
            holding[i] = holding[i] + addition
            surplus = surplus - addition
    return np.array([reach] + holding)


def ragged_sizes(rng, amount, total, limit, slope):
    if amount == 2:
        one = jax.random.randint(rng, (), max(1, total - limit), min(limit, total - 1) + 1)
        return jnp.stack([one, total - one])
    tallies = jnp.asarray(length_profile(amount, total, limit, slope), jnp.int32)
    pairs = (amount - 1) // 2
    giver, taker = tallies[1:1 + 2 * pairs:2], tallies[2:2 + 2 * pairs:2]
    slack = jnp.minimum(giver - 1, limit - taker)
    shifted = jax.random.randint(jax.random.fold_in(rng, 1), (pairs,), 0, 1 << 20) % (slack + 1)
    tallies = tallies.at[1:1 + 2 * pairs:2].set(giver - shifted).at[2:2 + 2 * pairs:2].set(taker + shifted)
    return tallies[jax.random.permutation(jax.random.fold_in(rng, 2), amount)]


def scatter_about(rng, extent, deviation, most, split=(), kind=jnp.bfloat16):
    values = deviation * jax.random.normal(rng, extent, jnp.float32)
    if split:
        values = values * steps_of(rng, extent, split, -0.22, 0.18)
    return jnp.clip(values, -most, most).astype(kind)


def setup_inputs(seed: int = 0) -> dict:
    seeds = jax.random.split(jax.random.key(seed), 10)
    return {
        "residuals": scatter_about(seeds[0], (SECTIONS, REPLICAS, TICKS, SEQ, D), 1.0, 6.0, ((0, 12), (1, 8), (3, 8))),
        "norm_gain": jnp.clip(1.0 + 0.1 * jax.random.normal(seeds[1], (SECTIONS, D), jnp.float32), 0.5, 1.5).astype(jnp.bfloat16),
        "projection": scatter_about(seeds[2], (SECTIONS, D, KVH, 2, HD), D ** -0.5, 0.0625, ((0, 12), (2, 8))),
        "queries": draw_queries(jax.random.fold_in(seeds[9], 71), 0),
        "output_grad": scatter_about(seeds[4], (SECTIONS, REPLICAS, TICKS, SEQ, KVH, GROUP * HD), 1.0, 6.0, ((0, 12), (1, 8), (4, 8))),
        "section_cotangent": scatter_about(seeds[5], (SECTIONS, REPLICAS, SEQ, D), 1.0, 6.0, ((0, 12), (1, 8), (2, 8))),
        "loss_cotangent": scatter_about(seeds[6], (REPLICAS, SEQ, D), 1.0, 6.0, ((0, 8), (1, 8))),
        "lengths": set_ends(jax.random.randint(seeds[7], (SECTIONS, REPLICAS, TICKS), SEQ // 2, SEQ + 1), jax.random.fold_in(seeds[7], 1), SEQ // 2, SEQ).astype(jnp.int32),
        "segments": jax.vmap(lambda own: jnp.searchsorted(jnp.cumsum(ragged_sizes(own, 3, SEQ, SEQ // 2, 1)), jnp.arange(SEQ), side="right"))(jax.random.split(seeds[8], SECTIONS * REPLICAS * TICKS)).reshape((SECTIONS, REPLICAS, TICKS, SEQ)).astype(jnp.int32),
    }


EPSILON = 1e-05
MASKED = -1e+30

def settle(tensor):
    return lax.optimization_barrier(tensor).astype(jnp.float32)

def attend_grad(query, key_rows, value_rows, masked_grad, visible):
    scaling = HD ** (-0.5)
    query_wide = settle(query)
    key_wide = settle(key_rows)
    value_wide = settle(value_rows)
    grad_wide = settle(masked_grad)
    scores = jnp.einsum('gqd,kd->gqk', query_wide, key_wide) * scaling
    scores = jnp.where(visible[None], scores, MASKED)
    row_max = lax.optimization_barrier(jnp.max(scores, axis=-1, keepdims=True))
    exponent = jnp.exp(scores - row_max)
    attention = exponent / lax.optimization_barrier(jnp.sum(exponent, axis=-1, keepdims=True))
    attention_wide = settle(attention.astype(jnp.bfloat16))
    mixed = jnp.einsum('gqk,kd->gqd', attention_wide, value_wide)
    correction = lax.optimization_barrier(jnp.sum(grad_wide * mixed, axis=-1))
    value_grad = jnp.einsum('gqk,gqd->kd', attention_wide, grad_wide)
    weight_grad = jnp.einsum('gqd,kd->gqk', grad_wide, value_wide)
    score_grad = settle((attention * (weight_grad - correction[..., None])).astype(jnp.bfloat16))
    query_grad = (jnp.einsum('gqk,kd->gqd', score_grad, key_wide) * scaling).astype(jnp.bfloat16)
    key_grad = jnp.einsum('gqk,gqd->kd', score_grad, query_wide) * scaling
    return (query_grad, jnp.concatenate([key_grad, value_grad], axis=1).astype(jnp.bfloat16))

def section_tick(residual, gain_row, weights, query_rows, grad_rows, length, segment):
    upcast = residual.astype(jnp.float32)
    inverse = lax.rsqrt(lax.optimization_barrier(jnp.mean(upcast * upcast, axis=1, keepdims=True)) + EPSILON)
    gain_wide = gain_row.astype(jnp.float32)
    normed = (upcast * inverse * gain_wide).astype(jnp.bfloat16)
    projected = jnp.dot(normed, weights, preferred_element_type=jnp.float32).astype(jnp.bfloat16)
    projected = projected.reshape(SEQ, KVH, 2, HD)
    position = jnp.arange(SEQ, dtype=jnp.int32)
    visible = (position[None, :] <= position[:, None]) & (segment[:, None] == segment[None, :])
    live_mask = (position < length).astype(jnp.bfloat16)
    masked_grad = grad_rows * live_mask[:, None, None]
    query_heads = query_rows.reshape(SEQ, KVH, GROUP, HD).transpose(1, 2, 0, 3)
    grad_heads = masked_grad.reshape(SEQ, KVH, GROUP, HD).transpose(1, 2, 0, 3)
    key_heads = projected[:, :, 0, :].transpose(1, 0, 2)
    value_heads = projected[:, :, 1, :].transpose(1, 0, 2)
    query_grad, pair_grad = jax.vmap(attend_grad, in_axes=(0, 0, 0, 0, None))(query_heads, key_heads, value_heads, grad_heads, visible)
    query_grad = query_grad.transpose(2, 0, 1, 3).reshape(SEQ, KVH, GROUP * HD)
    head_weights = weights.astype(jnp.float32).reshape(D, KVH, 2 * HD)
    partial_value = jnp.einsum('hsc,dhc->hsd', settle(pair_grad), head_weights)
    normed_grad = lax.optimization_barrier(jnp.sum(settle(partial_value.astype(jnp.bfloat16)), axis=0))
    scaled = normed_grad * gain_wide
    norm_back = inverse * scaled - upcast * inverse * inverse * inverse * lax.optimization_barrier(jnp.mean(scaled * upcast, axis=1, keepdims=True))
    pair_flat = pair_grad.transpose(1, 0, 2).reshape(SEQ, KVH * 2 * HD)
    return (query_grad, pair_flat, normed, norm_back)

def reference(residuals, norm_gain, projection, queries, output_grad, section_cotangent, loss_cotangent, lengths, segments):

    def first_pass(section_index):
        weights = projection[section_index].reshape(D, KVH * 2 * HD)

        def replica_pass(replica):
            outcome = section_tick(residuals[section_index, replica, 0], norm_gain[section_index], weights, queries[section_index, replica, 0], output_grad[section_index, replica, 0], lengths[section_index, replica, 0], segments[section_index, replica, 0])
            return (section_cotangent[section_index, replica].astype(jnp.float32) + outcome[3]).astype(jnp.bfloat16)
        return lax.map(replica_pass, jnp.arange(REPLICAS, dtype=jnp.int32))
    outgoing = lax.map(first_pass, jnp.arange(SECTIONS, dtype=jnp.int32))
    incoming = jnp.concatenate([outgoing[1:], loss_cotangent[None]], axis=0)

    def second_pass(section_index):
        weights = projection[section_index].reshape(D, KVH * 2 * HD)

        def replica_step(running, replica):
            query_list = []
            replica_sum = jnp.zeros((D, KVH * 2 * HD), jnp.float32)
            norm_last = None
            for tick_index in range(2):
                query_grad, pair_flat, normed, norm_back = section_tick(residuals[section_index, replica, tick_index], norm_gain[section_index], weights, queries[section_index, replica, tick_index], output_grad[section_index, replica, tick_index], lengths[section_index, replica, tick_index], segments[section_index, replica, tick_index])
                query_list.append(query_grad)
                replica_sum = replica_sum + jnp.dot(normed.T, pair_flat, preferred_element_type=jnp.float32)
                norm_last = norm_back
            running = running + settle(replica_sum.astype(jnp.bfloat16))
            residual_grad = (incoming[section_index, replica].astype(jnp.float32) + norm_last).astype(jnp.bfloat16)
            return (running, (jnp.stack(query_list), residual_grad))
        running, (query_all, residual_all) = lax.scan(replica_step, jnp.zeros((D, KVH * 2 * HD), jnp.float32), jnp.arange(REPLICAS, dtype=jnp.int32))
        return (running.astype(jnp.bfloat16).reshape(D, KVH, 2, HD), query_all, residual_all)
    projection_grad, query_grad, residual_grad = lax.map(second_pass, jnp.arange(SECTIONS, dtype=jnp.int32))
    return (query_grad, residual_grad, projection_grad)
```

```python
import jax
import jax.numpy as jnp
from jax import lax
from jax.sharding import Mesh
from jax.sharding import PartitionSpec as P

DP = ("dp_0", "dp_1")
EPSILON = 1e-05
MASKED = -1e30
LIFT = 256.0


def wide(value):
    return value.astype(jnp.float32)


def low(value):
    return value.astype(jnp.bfloat16)


def normalize(residual, gain_wide):
    upcast = wide(residual)
    inverse = lax.rsqrt(jnp.mean(upcast * upcast, axis=-1, keepdims=True) + EPSILON)
    return (low(upcast * inverse * gain_wide), inverse)


def head_grads(key_rows, value_rows, query_rows, grad_rows, length, segment):
    row_total, head_size = key_rows.shape
    group_size = query_rows.shape[-1] // head_size
    scaling = head_size ** (-0.5)
    position = lax.iota(jnp.int32, row_total)
    visible = (position[None, :] <= position[:, None]) & (segment[:, None] == segment[None, :])
    live_mask = (position < length).astype(jnp.bfloat16)
    query = query_rows.reshape(row_total, group_size, head_size)
    masked_grad = grad_rows.reshape(row_total, group_size, head_size) * live_mask[:, None, None]
    scores = (
        jnp.einsum("qgd,kd->gqk", query, key_rows, preferred_element_type=jnp.float32) * scaling
    )
    scores = jnp.where(visible[None], scores, MASKED)
    row_max = jnp.max(scores, axis=-1, keepdims=True)
    exponent = jnp.exp(scores - row_max)
    attention = exponent / jnp.sum(exponent, axis=-1, keepdims=True)
    attention_low = low(attention)
    mixed = jnp.einsum("gqk,kd->gqd", attention_low, value_rows, preferred_element_type=jnp.float32)
    correction = jnp.sum(mixed * wide(jnp.transpose(masked_grad, (1, 0, 2))), axis=-1)
    value_grad = jnp.einsum(
        "gqk,qgd->kd", attention_low, masked_grad, preferred_element_type=jnp.float32
    )
    weight_grad = jnp.einsum(
        "qgd,kd->gqk", masked_grad, value_rows, preferred_element_type=jnp.float32
    )
    score_grad = low(attention * (weight_grad - correction[..., None]))
    query_grad = low(
        jnp.einsum("gqk,kd->qgd", score_grad, key_rows, preferred_element_type=jnp.float32)
        * scaling
    )
    key_grad = (
        jnp.einsum("gqk,qgd->kd", score_grad, query, preferred_element_type=jnp.float32) * scaling
    )
    return (query_grad.reshape(row_total, 1, group_size * head_size), low(key_grad), low(value_grad))


def ring_shift(value, axis, step):
    count = lax.axis_size(axis)
    return lax.ppermute(value, axis, [(i, (i + step) % count) for i in range(count)])


def ring_sum(block, rows):
    def plus(arrived, own):
        return low(wide(arrived) + wide(own))

    far = block(4)
    up = ring_shift(far[:rows], "tensor", 1)
    down = ring_shift(far[rows:], "tensor", -1)
    near = block(3)
    up_sent = jnp.concatenate([plus(up, near[:rows]), near[rows:]])
    near = block(-3)
    down_sent = jnp.concatenate([near[:rows], plus(down, near[rows:])])
    for k in (2, 1):
        up = ring_shift(up_sent, "tensor", 1)
        down = ring_shift(down_sent, "tensor", -1)
        up_sent = plus(up, block(k))
        down_sent = plus(down, block(-k))
    up = ring_shift(up_sent, "tensor", 1)
    down = ring_shift(down_sent, "tensor", -1)
    return wide(block(0)) + wide(up) + wide(down)


def replica_total(term):
    width, columns = term.shape
    parts = term.reshape(4, width // 4, columns)
    arrived = lax.all_to_all(parts, "dp_0", split_axis=0, concat_axis=0, tiled=True)
    halves = wide(arrived).sum(axis=0).reshape(2, width // 8, columns)
    mine = lax.axis_index("dp_1")
    sent = low(lax.dynamic_index_in_dim(halves, 1 - mine, 0, keepdims=False))
    kept = lax.dynamic_index_in_dim(halves, mine, 0, keepdims=False)
    return low(kept + wide(lax.ppermute(sent, "dp_1", [(0, 1), (1, 0)])))


def on_device(
    residuals,
    norm_gain,
    projection,
    queries,
    output_grad,
    section_cotangent,
    loss_cotangent,
    lengths,
    segments,
):
    local_rows = residuals[0, 0]
    ticks, rows, model_width = local_rows.shape
    head_size = projection.shape[4]
    count = lax.axis_size("tensor")
    weights = projection[0, :, 0]
    gain_wide = wide(norm_gain[0])
    normed_local, inverse = normalize(local_rows, gain_wide)
    lifted = (wide(normed_local) * LIFT).astype(jnp.float16)
    gathered = lax.all_gather(
        lifted.reshape(ticks * rows, model_width), "tensor", axis=0, tiled=True
    )
    normed_all = low(wide(gathered) * (1.0 / LIFT))

    projected = low(
        jnp.einsum("rd,dkc->rkc", normed_all, weights, preferred_element_type=jnp.float32)
    ).reshape(count, ticks, rows, 2, head_size)

    outcomes = []
    for tick in range(ticks):
        pair = projected[:, tick].reshape(count * rows, 2, head_size)
        outcomes.append(
            head_grads(
                pair[:, 0],
                pair[:, 1],
                queries[0, 0, tick],
                output_grad[0, 0, tick],
                lengths[0, 0, tick],
                segments[0, 0, tick],
            )
        )

    def in_rows(which):
        stacked = jnp.stack([o[which].reshape(count, rows, head_size) for o in outcomes], axis=1)
        return stacked.reshape(count * ticks * rows, head_size)

    key_grad, value_grad = in_rows(1), in_rows(2)

    mine = lax.axis_index("tensor")
    pair_grad = jnp.stack([key_grad, value_grad], axis=1).reshape(count, ticks * rows, 2, head_size)
    rolled = jnp.roll(pair_grad, -mine, axis=0)
    terms = low(
        jnp.einsum("brkc,dkc->brd", rolled, weights, preferred_element_type=jnp.float32)
    )
    normed_grad = ring_sum(lambda k: terms[k % count], rows).reshape(ticks, rows, model_width)

    totals = []
    for grad in (value_grad, key_grad):
        term = low(
            lax.dot_general(
                normed_all, grad, (((0,), (0,)), ((), ())), preferred_element_type=jnp.float32
            )
        )
        totals.append(replica_total(term))
    projection_grad = jnp.stack([totals[1], totals[0]], axis=1)

    upcast = wide(local_rows)
    scaled = normed_grad * gain_wide
    norm_back = inverse * scaled - upcast * inverse * inverse * inverse * jnp.mean(
        scaled * upcast, axis=-1, keepdims=True
    )
    outgoing = low(wide(section_cotangent[0, 0]) + norm_back[0])
    sections = lax.axis_size("section")
    incoming = lax.ppermute(outgoing, "section", [(s, s - 1) for s in range(1, sections)])
    is_last = lax.axis_index("section") == sections - 1
    incoming = jnp.where(is_last, loss_cotangent[0], incoming)
    residual_grad = low(wide(incoming) + norm_back[1])
    query_all = jnp.stack([o[0] for o in outcomes])[None, None]
    return (query_all, residual_grad[None, None], projection_grad[None, :, None])


def solution(mesh):
    split = Mesh(
        mesh.devices.reshape(mesh.shape["section"], mesh.shape["tensor"], 4, 2),
        ("section", "tensor", "dp_0", "dp_1"),
    )
    placed = (
        P("section", DP, None, "tensor", None),
        P("section", None),
        P("section", None, "tensor", None, None),
        P("section", DP, None, None, "tensor", None),
        P("section", DP, None, None, "tensor", None),
        P("section", DP, "tensor", None),
        P(DP, "tensor", None),
        P("section", DP, None),
        P("section", DP, None, None),
    )
    return jax.shard_map(
        on_device,
        mesh=split,
        in_specs=placed,
        out_specs=(
            P("section", DP, None, None, "tensor", None),
            P("section", DP, "tensor", None),
            P("section", DP, "tensor", None, None),
        ),
        check_vma=False,
    )
```

```python
import functools

import jax
import jax.numpy as jnp
from jax import lax
from jax.experimental import pallas as pl
from jax.experimental.pallas import tpu as pltpu
from jax.sharding import Mesh
from jax.sharding import PartitionSpec as P

DP = ("dp_0", "dp_1")
EPSILON = 1e-05
MASKED = -1e30
LIFT = 256.0
FARTHEST = 3


def wide(value):
    return value.astype(jnp.float32)


def low(value):
    return value.astype(jnp.bfloat16)


def normalize(residual, gain_wide):
    upcast = wide(residual)
    inverse = lax.rsqrt(jnp.mean(upcast * upcast, axis=-1, keepdims=True) + EPSILON)
    return (low(upcast * inverse * gain_wide), inverse)


def dot(a, b, a_dim, b_dim):
    return lax.dot_general(
        a, b, (((a_dim,), (b_dim,)), ((), ())), preferred_element_type=jnp.float32
    )


def attention_body(
    scalars, segments, pairs, queries, grads, query_grad, pair_grad, pair_rolled, *, count, rows
):
    ticks, row_total, width = queries.shape
    head_size = pairs.shape[2]
    group_size = width // head_size
    scaling = head_size ** (-0.5)
    at_row = lax.broadcasted_iota(jnp.int32, (row_total, row_total), 0)
    at_column = lax.broadcasted_iota(jnp.int32, (row_total, row_total), 1)
    live_row = lax.broadcasted_iota(jnp.int32, (row_total, head_size), 0)
    mine = scalars[ticks]
    for tick in range(ticks):

        def plane(which):
            return jnp.concatenate(
                [
                    pairs[which, (owner * ticks + tick) * rows : (owner * ticks + tick + 1) * rows]
                    for owner in range(count)
                ],
                axis=0,
            )

        keys, values = plane(0), plane(1)
        segment = jnp.broadcast_to(wide(segments[tick : tick + 1]), (row_total, row_total))
        visible = (at_column <= at_row) & (segment == segment.T)
        live = low(wide(live_row < scalars[tick]))

        def stacked(ref):
            return jnp.concatenate(
                [ref[tick, :, h * head_size : (h + 1) * head_size] for h in range(group_size)],
                axis=0,
            )

        query = stacked(queries)
        masked = stacked(grads) * jnp.concatenate([live] * group_size, axis=0)
        scores = dot(query, keys, 1, 1) * scaling
        weight_grad = dot(masked, values, 1, 1)
        scores = jnp.where(jnp.concatenate([visible] * group_size, axis=0), scores, MASKED)
        exponent = jnp.exp(scores - jnp.max(scores, axis=-1, keepdims=True))
        attention = exponent / jnp.sum(exponent, axis=-1, keepdims=True)
        attention_low = low(attention)
        correction = jnp.sum(wide(attention_low) * weight_grad, axis=-1, keepdims=True)
        score_grad = low(attention * (weight_grad - correction))
        value_grad = dot(attention_low, masked, 0, 0)
        key_grad = dot(score_grad, query, 0, 0)
        query_term = low(dot(score_grad, keys, 1, 0) * scaling)
        for head in range(group_size):
            query_grad[tick, :, head * head_size : (head + 1) * head_size] = query_term[
                head * row_total : (head + 1) * row_total
            ]
        for which, grad in ((0, low(key_grad * scaling)), (1, low(value_grad))):
            for owner in range(count):
                piece = grad[owner * rows : (owner + 1) * rows]
                start = (owner * ticks + tick) * rows
                pair_grad[which, start : start + rows] = piece
                ahead = lax.rem(owner - mine - FARTHEST + 2 * count, count)
                place = pl.multiple_of((ahead * ticks + tick) * rows, rows)
                pair_rolled[which, pl.ds(place, rows)] = piece


def attention_grads(scalars, segments, pairs, queries, grads, count, rows):
    vmem = pl.BlockSpec(memory_space=pltpu.VMEM)
    return pl.pallas_call(
        functools.partial(attention_body, count=count, rows=rows),
        out_shape=(
            jax.ShapeDtypeStruct(queries.shape, jnp.bfloat16),
            jax.ShapeDtypeStruct(pairs.shape, jnp.bfloat16),
            jax.ShapeDtypeStruct(pairs.shape, jnp.bfloat16),
        ),
        in_specs=[pl.BlockSpec(memory_space=pltpu.SMEM)] + [vmem] * 4,
        out_specs=(vmem,) * 3,
        compiler_params=pltpu.CompilerParams(vmem_limit_bytes=16 << 20),
        name="attention_grads",
    )(scalars, segments, pairs, queries, grads)


def held_body(source, held, semaphore):
    copy = pltpu.make_async_copy(source, held, semaphore)
    copy.start()
    copy.wait()


def held(value):
    return pl.pallas_call(
        held_body,
        out_shape=pltpu.VMEM(value.shape, value.dtype),
        in_specs=[pl.BlockSpec(memory_space=pltpu.HBM)],
        out_specs=pl.BlockSpec(memory_space=pltpu.VMEM),
        scratch_shapes=[pltpu.SemaphoreType.DMA],
        compiler_params=pltpu.CompilerParams(vmem_limit_bytes=2 << 20),
        name="held",
    )(pltpu.with_memory_space_constraint(value, pltpu.HBM))


def ring_shift(value, axis, step):
    count = lax.axis_size(axis)
    return lax.ppermute(value, axis, [(i, (i + step) % count) for i in range(count)])


def replica_parts(term):
    width, columns = term.shape
    parts = term.reshape(4, width // 4, columns)
    arrived = lax.all_to_all(parts, "dp_0", split_axis=0, concat_axis=0, tiled=True)
    return arrived.reshape(4, 2, width // 8, columns)


def replica_swap(arrived):
    mine = lax.axis_index("dp_1")

    def total(half):
        return wide(lax.dynamic_index_in_dim(arrived, half, 1, keepdims=False)).sum(axis=0)

    sent = low(total(1 - mine))
    swapped = lax.ppermute(sent, "dp_1", [(0, 1), (1, 0)])
    return low(total(mine) + wide(swapped))


def layer(
    residuals,
    norm_gain,
    projection,
    queries,
    output_grad,
    section_cotangent,
    loss_cotangent,
    lengths,
    segments,
):
    local_rows = residuals[0, 0]
    ticks, rows, model_width = local_rows.shape
    count = lax.axis_size("tensor")
    weights = held(projection[0, :, 0])
    gain_wide = wide(norm_gain[0])
    normed_local, inverse = normalize(local_rows, gain_wide)
    lifted = (wide(normed_local) * LIFT).astype(jnp.float16)
    gathered = lax.all_gather(
        lifted.reshape(ticks * rows, model_width), "tensor", axis=0, tiled=True
    )
    normed_all = low(wide(gathered) * (1.0 / LIFT))

    pairs = low(jnp.einsum("rd,dkc->krc", normed_all, weights, preferred_element_type=jnp.float32))
    mine = lax.axis_index("tensor")
    scalars = jnp.concatenate([lengths[0, 0], mine[None].astype(jnp.int32)])
    query_grad, pair_grad, pair_rolled = attention_grads(
        scalars,
        segments[0, 0],
        pairs,
        queries[0, 0].reshape(ticks, count * rows, -1),
        output_grad[0, 0].reshape(ticks, count * rows, -1),
        count,
        rows,
    )

    def replica_term(which):
        return low(dot(normed_all, pair_grad[which], 0, 0))

    def terms(first, last):
        block = pair_rolled[:, first * ticks * rows : last * ticks * rows]
        value = low(jnp.einsum("krc,dkc->rd", block, weights, preferred_element_type=jnp.float32))
        return value.reshape(last - first, ticks * rows, model_width)

    def plus(arrived, own):
        return low(wide(arrived) + wide(own))

    arrived_v = replica_parts(replica_term(1))
    far = terms(0, 3)
    up = ring_shift(far[1, :rows], "tensor", 1)
    down = ring_shift(far[1, rows:], "tensor", -1)
    up = ring_shift(jnp.concatenate([plus(up, far[0, :rows]), far[0, rows:]]), "tensor", 1)
    down = ring_shift(jnp.concatenate([far[2, :rows], plus(down, far[2, rows:])]), "tensor", -1)
    arrived_k = replica_parts(replica_term(0))
    near = terms(3, 8)
    up = ring_shift(plus(up, near[4]), "tensor", 1)
    down = ring_shift(plus(down, near[0]), "tensor", -1)
    up = ring_shift(plus(up, near[3]), "tensor", 1)
    down = ring_shift(plus(down, near[1]), "tensor", -1)
    normed_grad = (wide(near[2]) + wide(up) + wide(down)).reshape(ticks, rows, model_width)

    totals = [replica_swap(arrived_v), replica_swap(arrived_k)]
    projection_grad = jnp.stack([totals[1], totals[0]], axis=1)

    upcast = wide(local_rows)
    scaled = normed_grad * gain_wide
    norm_back = inverse * scaled - upcast * inverse * inverse * inverse * jnp.mean(
        scaled * upcast, axis=-1, keepdims=True
    )
    outgoing = low(wide(section_cotangent[0, 0]) + norm_back[0])
    sections = lax.axis_size("section")
    incoming = lax.ppermute(outgoing, "section", [(s, s - 1) for s in range(1, sections)])
    is_last = lax.axis_index("section") == sections - 1
    incoming = jnp.where(is_last, loss_cotangent[0], incoming)
    residual_grad = low(wide(incoming) + norm_back[1])
    query_all = query_grad.reshape(queries.shape)
    return (query_all, residual_grad[None, None], projection_grad[None, :, None])


def solution(mesh):
    split = Mesh(
        mesh.devices.reshape(mesh.shape["section"], mesh.shape["tensor"], 4, 2),
        ("section", "tensor", "dp_0", "dp_1"),
    )
    placed = (
        P("section", DP, None, "tensor", None),
        P("section", None),
        P("section", None, "tensor", None, None),
        P("section", DP, None, None, "tensor", None),
        P("section", DP, None, None, "tensor", None),
        P("section", DP, "tensor", None),
        P(DP, "tensor", None),
        P("section", DP, None),
        P("section", DP, None, None),
    )
    return jax.shard_map(
        layer,
        mesh=split,
        in_specs=placed,
        out_specs=(
            P("section", DP, None, None, "tensor", None),
            P("section", DP, "tensor", None),
            P("section", DP, "tensor", None, None),
        ),
        check_vma=False,
    )
```

```python
import functools

import jax
import jax.numpy as jnp
from jax import lax
from jax.experimental import pallas as pl
from jax.experimental.pallas import tpu as pltpu
from jax.sharding import Mesh
from jax.sharding import PartitionSpec as P

DP = ("dp_0", "dp_1")
EPSILON = 1e-05
MASKED = -1e30
LIFT = 256.0
FARTHEST = 3


def wide(value):
    return value.astype(jnp.float32)


def low(value):
    return value.astype(jnp.bfloat16)


def normalize(residual, gain_wide):
    upcast = wide(residual)
    inverse = lax.rsqrt(jnp.mean(upcast * upcast, axis=-1, keepdims=True) + EPSILON)
    return (low(upcast * inverse * gain_wide), inverse)


def dot(a, b, a_dim, b_dim):
    return lax.dot_general(
        a, b, (((a_dim,), (b_dim,)), ((), ())), preferred_element_type=jnp.float32
    )


def attention_body(
    lengths, segments, pairs, queries, grads, query_grad, pair_grad, pair_rolled, *, count, rows
):
    ticks, row_total, width = queries.shape
    head_size = pairs.shape[2]
    group_size = width // head_size
    scaling = head_size ** (-0.5)
    at_row = lax.broadcasted_iota(jnp.int32, (row_total, row_total), 0)
    at_column = lax.broadcasted_iota(jnp.int32, (row_total, row_total), 1)
    live_row = lax.broadcasted_iota(jnp.int32, (row_total, head_size), 0)
    mine = lax.axis_index("tensor")
    for tick in range(ticks):

        def plane(which):
            return jnp.concatenate(
                [
                    pairs[which, (owner * ticks + tick) * rows : (owner * ticks + tick + 1) * rows]
                    for owner in range(count)
                ],
                axis=0,
            )

        keys, values = plane(0), plane(1)
        segment = jnp.broadcast_to(wide(segments[tick : tick + 1]), (row_total, row_total))
        visible = (at_column <= at_row) & (segment == segment.T)
        live = low(wide(live_row < lengths[tick]))

        def stacked(ref):
            return jnp.concatenate(
                [ref[tick, :, h * head_size : (h + 1) * head_size] for h in range(group_size)],
                axis=0,
            )

        query = stacked(queries)
        masked = stacked(grads) * jnp.concatenate([live] * group_size, axis=0)
        scores = dot(query, keys, 1, 1) * scaling
        weight_grad = dot(masked, values, 1, 1)
        scores = jnp.where(jnp.concatenate([visible] * group_size, axis=0), scores, MASKED)
        exponent = jnp.exp(scores - jnp.max(scores, axis=-1, keepdims=True))
        attention = exponent / jnp.sum(exponent, axis=-1, keepdims=True)
        attention_low = low(attention)
        correction = jnp.sum(wide(attention_low) * weight_grad, axis=-1, keepdims=True)
        score_grad = low(attention * (weight_grad - correction))
        value_grad = dot(attention_low, masked, 0, 0)
        key_grad = dot(score_grad, query, 0, 0)
        query_term = low(dot(score_grad, keys, 1, 0) * scaling)
        for head in range(group_size):
            query_grad[tick, :, head * head_size : (head + 1) * head_size] = query_term[
                head * row_total : (head + 1) * row_total
            ]
        for which, grad in ((0, low(key_grad * scaling)), (1, low(value_grad))):
            for owner in range(count):
                piece = grad[owner * rows : (owner + 1) * rows]
                start = (owner * ticks + tick) * rows
                pair_grad[which, start : start + rows] = piece
                ahead = lax.rem(owner - mine - FARTHEST + 2 * count, count)
                place = pl.multiple_of((ahead * ticks + tick) * rows, rows)
                pair_rolled[which, pl.ds(place, rows)] = piece


def attention_grads(lengths, segments, pairs, queries, grads, count, rows):
    vmem = pl.BlockSpec(memory_space=pltpu.VMEM)
    return pl.pallas_call(
        functools.partial(attention_body, count=count, rows=rows),
        out_shape=(
            jax.ShapeDtypeStruct(queries.shape, jnp.bfloat16),
            jax.ShapeDtypeStruct(pairs.shape, jnp.bfloat16),
            jax.ShapeDtypeStruct(pairs.shape, jnp.bfloat16),
        ),
        in_specs=[pl.BlockSpec(memory_space=pltpu.SMEM)] + [vmem] * 4,
        out_specs=(vmem,) * 3,
        compiler_params=pltpu.CompilerParams(vmem_limit_bytes=16 << 20),
        name="attention_grads",
    )(lengths, segments, pairs, queries, grads)


def ring_shift(value, axis, step):
    count = lax.axis_size(axis)
    return lax.ppermute(value, axis, [(i, (i + step) % count) for i in range(count)])


def replica_parts(term, own):
    width, columns = term.shape
    quarter, half = width // 4, width // 8

    def part(at, length):
        return lax.dynamic_slice(
            term, (own[at], own[5]), (length, columns), allow_negative_indices=False
        )

    others = [ring_shift(part(k, quarter), "dp_0", k) for k in (1, 3, 2)]
    return [part(0, half), part(4, half)] + others


def replica_sum(parts, upper):
    half = parts[0].shape[0]
    low_half, high_half = (
        wide(parts[index]) + sum(wide(other[at : at + half]) for other in parts[2:])
        for index, at in ((0, 0), (1, half))
    )
    return low(jnp.where(upper, low_half, high_half)), jnp.where(upper, high_half, low_half)


def swapped(value):
    return wide(lax.ppermute(value, "dp_1", [(0, 1), (1, 0)]))


def layer(
    residuals,
    norm_gain,
    projection,
    queries,
    output_grad,
    section_cotangent,
    loss_cotangent,
    lengths,
    segments,
):
    _, _, ticks, rows, model_width = residuals.shape
    local_rows = residuals.reshape(ticks * rows, model_width)
    count = lax.axis_size("tensor")
    sections = lax.axis_size("section")
    weights = projection[0, :, 0]
    gain_wide = wide(norm_gain[0])
    normed_local, inverse = normalize(local_rows, gain_wide)
    lifted = (wide(normed_local) * LIFT).astype(jnp.float16)
    place = lax.axis_index("dp_0")
    own = [((place + k) & 3) * (model_width // 4) for k in range(4)]
    own = own + [own[0] + model_width // 8, jnp.zeros((), jnp.int32)]
    upper = lax.axis_index("dp_1") == 1
    is_last = lax.axis_index("section") == sections - 1
    lifted, own, upper, is_last = lax.optimization_barrier((lifted, own, upper, is_last))
    gathered = lax.all_gather(lifted, "tensor", axis=0, tiled=True)
    normed_all = low(wide(gathered) * (1.0 / LIFT))

    pairs = low(jnp.einsum("rd,dkc->krc", normed_all, weights, preferred_element_type=jnp.float32))
    query_grad, pair_grad, pair_rolled = attention_grads(
        lengths[0, 0],
        segments[0, 0],
        pairs,
        queries[0, 0].reshape(ticks, count * rows, -1),
        output_grad[0, 0].reshape(ticks, count * rows, -1),
        count,
        rows,
    )

    def replica_term(which):
        return low(dot(normed_all, pair_grad[which], 0, 0))

    def plus(arrived, mine):
        return low(wide(arrived) + wide(mine))

    terms = low(
        jnp.einsum("krc,dkc->rd", pair_rolled, weights, preferred_element_type=jnp.float32)
    ).reshape(count, ticks * rows, model_width)

    def term(ahead):
        return terms[(ahead - FARTHEST) % count]

    sent_v, kept_v = replica_sum(replica_parts(replica_term(1), own), upper)
    parts_k = replica_parts(replica_term(0), own)
    parts_k, _ = lax.optimization_barrier((parts_k, sent_v))
    sent_k, kept_k = replica_sum(parts_k, upper)
    across = ring_shift(term(4), "tensor", 4)
    up = ring_shift(term(3), "tensor", 1)
    down = ring_shift(term(-3), "tensor", -1)
    up = ring_shift(plus(up, term(2)), "tensor", 1)
    down = ring_shift(plus(down, term(-2)), "tensor", -1)
    up = ring_shift(plus(up, term(1)), "tensor", 1)
    down = ring_shift(plus(down, term(-1)), "tensor", -1)
    normed_grad = wide(term(0)) + wide(up) + wide(down) + wide(across)

    values_total = low(kept_v + swapped(sent_v))
    keys_total = low(kept_k + swapped(sent_k))
    projection_grad = jnp.stack([keys_total, values_total], axis=1)

    upcast = wide(local_rows)
    scaled = normed_grad * gain_wide
    norm_back = inverse * scaled - upcast * inverse * inverse * inverse * jnp.mean(
        scaled * upcast, axis=-1, keepdims=True
    )
    outgoing = low(wide(section_cotangent[0, 0]) + norm_back[:rows])
    incoming = lax.ppermute(outgoing, "section", [(s, s - 1) for s in range(1, sections)])
    incoming = jnp.where(is_last, loss_cotangent[0], incoming)
    residual_grad = low(wide(incoming) + norm_back[rows:])
    query_all = query_grad.reshape(queries.shape)
    return (query_all, residual_grad[None, None], projection_grad[None, :, None])


def solution(mesh):
    split = Mesh(
        mesh.devices.reshape(mesh.shape["section"], mesh.shape["tensor"], 4, 2),
        ("section", "tensor", "dp_0", "dp_1"),
    )
    placed = (
        P("section", DP, None, "tensor", None),
        P("section", None),
        P("section", None, "tensor", None, None),
        P("section", DP, None, None, "tensor", None),
        P("section", DP, None, None, "tensor", None),
        P("section", DP, "tensor", None),
        P(DP, "tensor", None),
        P("section", DP, None),
        P("section", DP, None, None),
    )
    return jax.shard_map(
        layer,
        mesh=split,
        in_specs=placed,
        out_specs=(
            P("section", DP, None, None, "tensor", None),
            P("section", DP, "tensor", None),
            P("section", DP, "tensor", None, None),
        ),
        check_vma=False,
    )
```

```python
import functools

import jax
import jax.numpy as jnp
from jax import lax
from jax.experimental import pallas as pl
from jax.experimental.pallas import tpu as pltpu
from jax.sharding import Mesh
from jax.sharding import PartitionSpec as P

DP = ("dp_0", "dp_1")
EPSILON = 1e-05
MASKED = -1e30
LIFT = 256.0
FARTHEST = 3


def wide(value):
    return value.astype(jnp.float32)


def low(value):
    return value.astype(jnp.bfloat16)


def normalize(residual, gain_wide):
    upcast = wide(residual)
    inverse = lax.rsqrt(jnp.mean(upcast * upcast, axis=-1, keepdims=True) + EPSILON)
    return (low(upcast * inverse * gain_wide), inverse)


def dot(a, b, a_dim, b_dim):
    return lax.dot_general(
        a, b, (((a_dim,), (b_dim,)), ((), ())), preferred_element_type=jnp.float32
    )


def attention_body(
    lengths, segments, pairs, queries, grads, query_grad, pair_grad, pair_rolled, *, count, rows
):
    ticks, row_total, width = queries.shape
    head_size = pairs.shape[2]
    group_size = width // head_size
    scaling = head_size ** (-0.5)
    at_row = lax.broadcasted_iota(jnp.int32, (row_total, row_total), 0)
    at_column = lax.broadcasted_iota(jnp.int32, (row_total, row_total), 1)
    live_row = lax.broadcasted_iota(jnp.int32, (row_total, head_size), 0)
    mine = lax.axis_index("tensor")
    for tick in range(ticks):

        def plane(which):
            return jnp.concatenate(
                [
                    pairs[which, (owner * ticks + tick) * rows : (owner * ticks + tick + 1) * rows]
                    for owner in range(count)
                ],
                axis=0,
            )

        keys, values = plane(0), plane(1)
        segment = jnp.broadcast_to(wide(segments[tick : tick + 1]), (row_total, row_total))
        visible = (at_column <= at_row) & (segment == segment.T)
        live = low(wide(live_row < lengths[tick]))

        def stacked(ref):
            return jnp.concatenate(
                [ref[tick, :, h * head_size : (h + 1) * head_size] for h in range(group_size)],
                axis=0,
            )

        query = stacked(queries)
        masked = stacked(grads) * jnp.concatenate([live] * group_size, axis=0)
        scores = dot(query, keys, 1, 1) * scaling
        weight_grad = dot(masked, values, 1, 1)
        scores = jnp.where(jnp.concatenate([visible] * group_size, axis=0), scores, MASKED)
        exponent = jnp.exp(scores - jnp.max(scores, axis=-1, keepdims=True))
        attention = exponent / jnp.sum(exponent, axis=-1, keepdims=True)
        attention_low = low(attention)
        correction = jnp.sum(wide(attention_low) * weight_grad, axis=-1, keepdims=True)
        score_grad = low(attention * (weight_grad - correction))
        value_grad = dot(attention_low, masked, 0, 0)
        key_grad = dot(score_grad, query, 0, 0)
        query_term = low(dot(score_grad, keys, 1, 0) * scaling)
        for head in range(group_size):
            query_grad[tick, :, head * head_size : (head + 1) * head_size] = query_term[
                head * row_total : (head + 1) * row_total
            ]
        for which, grad in ((0, low(key_grad * scaling)), (1, low(value_grad))):
            for owner in range(count):
                piece = grad[owner * rows : (owner + 1) * rows]
                start = (owner * ticks + tick) * rows
                pair_grad[which, start : start + rows] = piece
                ahead = lax.rem(owner - mine - FARTHEST + 2 * count, count)
                place = pl.multiple_of((ahead * ticks + tick) * rows, rows)
                pair_rolled[which, pl.ds(place, rows)] = piece


def attention_grads(lengths, segments, pairs, queries, grads, count, rows):
    vmem = pl.BlockSpec(memory_space=pltpu.VMEM)
    return pl.pallas_call(
        functools.partial(attention_body, count=count, rows=rows),
        out_shape=(
            jax.ShapeDtypeStruct(queries.shape, jnp.bfloat16),
            jax.ShapeDtypeStruct(pairs.shape, jnp.bfloat16),
            jax.ShapeDtypeStruct(pairs.shape, jnp.bfloat16),
        ),
        in_specs=[pl.BlockSpec(memory_space=pltpu.SMEM)] + [vmem] * 4,
        out_specs=(vmem,) * 3,
        compiler_params=pltpu.CompilerParams(vmem_limit_bytes=16 << 20),
        name="attention_grads",
    )(lengths, segments, pairs, queries, grads)


def ring_shift(value, axis, step):
    count = lax.axis_size(axis)
    return lax.ppermute(value, axis, [(i, (i + step) % count) for i in range(count)])


def replica_parts(term, own):
    width, columns = term.shape
    quarter, half = width // 4, width // 8

    def part(at, length):
        return lax.dynamic_slice(
            term, (own[at], own[5]), (length, columns), allow_negative_indices=False
        )

    others = [ring_shift(part(k, quarter), "dp_0", k) for k in (1, 3, 2)]
    return [part(0, half), part(4, half)] + others


def replica_sum(parts, upper):
    half = parts[0].shape[0]
    low_half, high_half = (
        wide(parts[index]) + sum(wide(other[at : at + half]) for other in parts[2:])
        for index, at in ((0, 0), (1, half))
    )
    return low(jnp.where(upper, low_half, high_half)), jnp.where(upper, high_half, low_half)


def swapped(value):
    return wide(lax.ppermute(value, "dp_1", [(0, 1), (1, 0)]))


def layer(
    residuals,
    norm_gain,
    projection,
    queries,
    output_grad,
    section_cotangent,
    loss_cotangent,
    lengths,
    segments,
):
    _, _, ticks, rows, model_width = residuals.shape
    local_rows = residuals.reshape(ticks * rows, model_width)
    count = lax.axis_size("tensor")
    sections = lax.axis_size("section")
    weights = projection[0, :, 0]
    gain_wide = wide(norm_gain[0])
    normed_local, inverse = normalize(local_rows, gain_wide)
    lifted = (wide(normed_local) * LIFT).astype(jnp.float16)
    place = lax.axis_index("dp_0")
    own = [((place + k) & 3) * (model_width // 4) for k in range(4)]
    own = own + [own[0] + model_width // 8, jnp.zeros((), jnp.int32)]
    upper = lax.axis_index("dp_1") == 1
    is_last = lax.axis_index("section") == sections - 1
    lifted, own, upper, is_last = lax.optimization_barrier((lifted, own, upper, is_last))
    gathered = lax.all_gather(lifted, "tensor", axis=0, tiled=True)
    normed_all = low(wide(gathered) * (1.0 / LIFT))

    pairs = low(jnp.einsum("rd,dkc->krc", normed_all, weights, preferred_element_type=jnp.float32))
    query_grad, pair_grad, pair_rolled = attention_grads(
        lengths[0, 0],
        segments[0, 0],
        pairs,
        queries[0, 0].reshape(ticks, count * rows, -1),
        output_grad[0, 0].reshape(ticks, count * rows, -1),
        count,
        rows,
    )

    def replica_term(which):
        return low(dot(normed_all, pair_grad[which], 0, 0))

    def plus(arrived, mine):
        return low(wide(arrived) + wide(mine))

    terms = low(
        jnp.einsum("krc,dkc->rd", pair_rolled, weights, preferred_element_type=jnp.float32)
    ).reshape(count, ticks * rows, model_width)

    def term(ahead):
        return terms[(ahead - FARTHEST) % count]

    sent_v, kept_v = replica_sum(replica_parts(replica_term(1), own), upper)
    parts_k = replica_parts(replica_term(0), own)
    parts_k, _ = lax.optimization_barrier((parts_k, sent_v))
    sent_k, kept_k = replica_sum(parts_k, upper)
    up = ring_shift(term(4), "tensor", 1)
    up = ring_shift(plus(up, term(3)), "tensor", 1)
    down = ring_shift(term(-3), "tensor", -1)
    up = ring_shift(plus(up, term(2)), "tensor", 1)
    down = ring_shift(plus(down, term(-2)), "tensor", -1)
    up = ring_shift(plus(up, term(1)), "tensor", 1)
    down = ring_shift(plus(down, term(-1)), "tensor", -1)
    normed_grad = wide(term(0)) + wide(up) + wide(down)

    values_total = low(kept_v + swapped(sent_v))
    keys_total = low(kept_k + swapped(sent_k))
    projection_grad = jnp.stack([keys_total, values_total], axis=1)

    upcast = wide(local_rows)
    scaled = normed_grad * gain_wide
    norm_back = inverse * scaled - upcast * inverse * inverse * inverse * jnp.mean(
        scaled * upcast, axis=-1, keepdims=True
    )
    outgoing = low(wide(section_cotangent[0, 0]) + norm_back[:rows])
    incoming = lax.ppermute(outgoing, "section", [(s, s - 1) for s in range(1, sections)])
    incoming = jnp.where(is_last, loss_cotangent[0], incoming)
    residual_grad = low(wide(incoming) + norm_back[rows:])
    query_all = query_grad.reshape(queries.shape)
    return (query_all, residual_grad[None, None], projection_grad[None, :, None])


def solution(mesh):
    split = Mesh(
        mesh.devices.reshape(mesh.shape["section"], mesh.shape["tensor"], 4, 2),
        ("section", "tensor", "dp_0", "dp_1"),
    )
    placed = (
        P("section", DP, None, "tensor", None),
        P("section", None),
        P("section", None, "tensor", None, None),
        P("section", DP, None, None, "tensor", None),
        P("section", DP, None, None, "tensor", None),
        P("section", DP, "tensor", None),
        P(DP, "tensor", None),
        P("section", DP, None),
        P("section", DP, None, None),
    )
    return jax.shard_map(
        layer,
        mesh=split,
        in_specs=placed,
        out_specs=(
            P("section", DP, None, None, "tensor", None),
            P("section", DP, "tensor", None),
            P("section", DP, "tensor", None, None),
        ),
        check_vma=False,
    )
```
